128 devices in a mesh: parts: 1, data: 128 (over z, y, x, core).
Axes of the slice: x: 4, y: 4, z: 4, core: 2. Of those that a mesh axis runs over, the one named last changes fastest.
Arguments:
- feat_rows: bfloat16 [1048576, 28], P('data')
- labels: int32 [1048576], P('data')
- pos_init: float32 [28, 64], P(None, 'parts')
- mom_init: float32 [28, 64], P(None, 'parts')
- step_sizes: float32 [64, 64], P(None, 'parts')
Outputs:
- output 1: float32 [28, 64], P(None, 'parts')
- output 2: float32 [28, 64], P(None, 'parts')
- output 3: float32 [64, 64], P(None, 'parts')
All inputs are finite; a program needn't handle non-finite values.
Results may differ from the reference program's by a relative error of at most 0.00335409.
Values are sent between devices in bfloat16 or wider.
A program may use at most 1 GiB of HBM per device.

```python
import jax
import jax.numpy as jnp
from jax import lax

ROWS_DEV = 8192
GROUP_DEVS = 128
FEATURES = 28
CHAINS = 64
LEAPFROG = 64

ROWS_TOTAL = ROWS_DEV * GROUP_DEVS
PRIOR_VAR = 4.0
STEP_BASE = (ROWS_DEV + ROWS_TOTAL / FEATURES) ** -0.5
MOM_SCALE = (ROWS_TOTAL / FEATURES) ** 0.5


def setup_inputs(seed: int = 0, part: int = 0) -> dict:
    base_key = jax.random.key(seed)
    key_rate, key_label, key_noise, key_dir, key_strong = jax.random.split(base_key, 5)
    part_key = jax.random.fold_in(jax.random.key(seed + 1), part)
    key_pos, key_mom, key_step = jax.random.split(part_key, 3)
    shard_of_row = jnp.arange(ROWS_TOTAL) // ROWS_DEV
    label_rate = jax.random.randint(key_rate, (GROUP_DEVS,), 1, 16)
    label_draws = jax.random.randint(key_label, (ROWS_TOTAL,), 0, 16)
    labels = (label_draws < label_rate[shard_of_row]).astype(jnp.int32)
    label_sign = (2 * labels - 1).astype(jnp.float32)
    direction = jax.random.normal(key_dir, (FEATURES,), jnp.float32)
    noise_vals = jax.random.normal(key_noise, (ROWS_TOTAL, FEATURES), jnp.float32)
    noise_part = (0.5 / FEATURES ** 0.5) * (noise_vals + label_sign[:, None] * direction[None, :] / FEATURES ** 0.5)
    col_index = jnp.arange(FEATURES)
    strong_mask = ((col_index[None, :] % GROUP_DEVS) == (shard_of_row[:, None] % FEATURES)).astype(jnp.float32)
    strong_count = jnp.sum(strong_mask, axis=1, keepdims=True)
    strong_vals = 1.0 + 0.5 * jax.random.normal(key_strong, (ROWS_TOTAL, FEATURES), jnp.float32)
    feat_rows = (noise_part + strong_mask * strong_vals / jnp.sqrt(strong_count)).astype(jnp.bfloat16)
    pos_init = 0.5 * jax.random.normal(key_pos, (FEATURES, CHAINS), jnp.float32)
    mom_init = (0.5 * MOM_SCALE) * jax.random.normal(key_mom, (FEATURES, CHAINS), jnp.float32)
    step_sizes = STEP_BASE * jax.random.uniform(key_step, (LEAPFROG, CHAINS), jnp.float32, 0.6, 0.9)
    return {"feat_rows": feat_rows, "labels": labels, "pos_init": pos_init, "mom_init": mom_init, "step_sizes": step_sizes}


def potential_terms(feat_rows, labels, positions):
    pos_half = positions.astype(jnp.bfloat16)
    feat_blocks = feat_rows.reshape(GROUP_DEVS, ROWS_DEV, FEATURES)
    label_blocks = labels.astype(jnp.float32).reshape(GROUP_DEVS, ROWS_DEV, 1)

    def block_step(running, block_in):
        grad_acc, loss_acc = running
        block_rows, block_labels = block_in
        logits = jnp.dot(block_rows, pos_half, preferred_element_type=jnp.float32)
        residual = (block_labels - jax.nn.sigmoid(logits)).astype(jnp.bfloat16)
        grad_acc = grad_acc + jnp.dot(block_rows.T, residual, preferred_element_type=jnp.float32)
        loss_acc = loss_acc + jnp.sum(jax.nn.softplus(logits) - block_labels * logits, axis=0)
        return (grad_acc, loss_acc), None

    zero_state = (jnp.zeros((FEATURES, CHAINS), jnp.float32), jnp.zeros((CHAINS,), jnp.float32))
    (grad_lik, loss_lik), _ = lax.scan(block_step, zero_state, (feat_blocks, label_blocks))
    gradient = grad_lik - positions / PRIOR_VAR
    potential = loss_lik + jnp.sum(positions * positions, axis=0) / (2.0 * PRIOR_VAR)
    return gradient, potential


def reference(feat_rows, labels, pos_init, mom_init, step_sizes):
    grad_init, _ = potential_terms(feat_rows, labels, pos_init)

    def leap_step(loop_state, step_size):
        positions, momentum, gradient = loop_state
        momentum = momentum + 0.5 * step_size * gradient
        positions = positions + step_size * momentum
        gradient, potential = potential_terms(feat_rows, labels, positions)
        momentum = momentum + 0.5 * step_size * gradient
        energy = potential + 0.5 * jnp.sum(momentum * momentum, axis=0)
        return (positions, momentum, gradient), energy

    (positions, momentum, _), energies = lax.scan(leap_step, (pos_init, mom_init, grad_init), step_sizes)
    return positions, momentum, energies
```

```python
import itertools

import jax
import jax.numpy as jnp
from jax import lax
from jax.experimental import pallas as pl
from jax.experimental.pallas import tpu as pltpu
from jax.sharding import PartitionSpec as P

PRIOR_VAR = 4.0
FEATURES = 28
STEPS = 64
CHAINS = 64
HALF = 32
ROWS = 8192
PACK = 8
PROWS = ROWS // PACK
CHUNK = 256
GROUP = 64
MESSAGE = 7
OFFSETS = list(itertools.product(range(4), repeat=3))


def hops(offset):
    return sum(min(step, 4 - step) for step in offset)


FAR_FIRST = sorted(range(1, 64), key=lambda k: -hops(OFFSETS[k]))


def ring_sum(values):
    if len(values) == 1:
        return values[0]
    quarter = len(values) // 4
    part = [ring_sum(values[i * quarter:(i + 1) * quarter]) for i in range(4)]
    return (part[0] + part[2]) + (part[1] + part[3])


def chain_kernel(rows_ref, pos_ref, mom_ref, eps_ref, out_ref,
                 packed, packed_t, weights, resid, outgoing, incoming, loss_rows, kin_rows,
                 energy_out, energy_in, final,
                 send_sem, recv_sem, esend_sem, erecv_sem, pair_send, pair_recv):
    index = lax.axis_index("data")
    core = index % 2
    x, y, z = (index // 2) % 4, (index // 8) % 4, index // 32
    partner = (0, index + 1 - 2 * core)

    def peer(offset):
        return (0, ((((z + offset[0]) % 4) * 4 + (y + offset[1]) % 4) * 4 + (x + offset[2]) % 4) * 2 + core)

    lane = lax.broadcasted_iota(jnp.int32, (8, 128), 1) // HALF
    lane16 = lax.broadcasted_iota(jnp.int32, (16, 128), 1) // HALF
    real_row = lax.broadcasted_iota(jnp.int32, (8, 128), 0) < MESSAGE

    def pair_copy(ref, src, dst, slot):
        return pltpu.make_async_remote_copy(src_ref=ref.at[src], dst_ref=ref.at[dst], send_sem=pair_send.at[slot], recv_sem=pair_recv.at[slot], device_id=partner, device_id_type=pl.DeviceIdType.MESH)

    column = lax.broadcasted_iota(jnp.int32, (FEATURES, 256), 1)
    feature = lax.broadcasted_iota(jnp.int32, (FEATURES, 256), 0)
    wanted = ((column % 32) // 8) * 7 + column % 8
    place = (feature == wanted) & (column % 8 < 7)
    for r in range(PROWS // CHUNK):
        acc = jnp.zeros((CHUNK, 256), jnp.float32)
        for g in range(PACK):
            place_g = jnp.where(place & (column // 32 == g), 1.0, 0.0).astype(jnp.bfloat16)
            acc = acc + jnp.dot(rows_ref[g * PROWS + r * CHUNK:g * PROWS + (r + 1) * CHUNK, :], place_g, preferred_element_type=jnp.float32)
        packed[0, r * CHUNK:(r + 1) * CHUNK, :] = acc.astype(jnp.bfloat16)
        packed_t[0, :, r * CHUNK:(r + 1) * CHUNK] = acc.T.astype(jnp.bfloat16)
    pair_copy(packed, 0, 1, 0).start()
    pair_copy(packed_t, 0, 1, 1).start()
    weights[...] = jnp.zeros_like(weights)
    pair_copy(packed, 0, 1, 0).wait()
    pair_copy(packed_t, 0, 1, 1).wait()

    def lane_total(row):
        row = row + pltpu.roll(row, 64, 1)
        return row + pltpu.roll(row, 32, 1)

    def evaluate(positions, parity, loss_index, last):
        half = positions.astype(jnp.bfloat16).astype(jnp.float32) * 0.5
        turned = [half] + [pltpu.roll(half, 32 * k, 1) for k in range(1, 4)]
        for j in range(4):
            for p in range(2):
                block = jnp.concatenate([turned[(j - 2 * p) % 4], turned[(j - 2 * p - 1) % 4]], axis=0)
                block = jnp.where(lane16 == j, block, 0.0).astype(jnp.bfloat16)
                for h in range(2):
                    row = 32 * (4 * h + j) + 16 * p
                    weights[row:row + 16, 128 * h:128 * (h + 1)] = block
        linear = jnp.zeros((8, 256), jnp.float32)
        logs = jnp.zeros((8, 256), jnp.float32)
        grads = [None, None]
        product = None
        count = 0
        for b in range(2):
            for r in range(PROWS // CHUNK):
                span = slice(r * CHUNK, (r + 1) * CHUNK)
                logit = jnp.dot(packed[b, span, :], weights[...], preferred_element_type=jnp.float32)
                bent = jnp.tanh(logit)
                part = (1.0 + bent).astype(jnp.bfloat16)
                for h in range(2):
                    cols = slice(128 * h, 128 * (h + 1))
                    piece = jnp.dot(packed_t[b, cols, span], part[:, cols], preferred_element_type=jnp.float32)
                    grads[h] = piece if grads[h] is None else grads[h] + piece
                factor = 1.0 + jnp.abs(bent)
                positive = jnp.maximum(logit, 0.0)
                for i in range(CHUNK // 8):
                    rows8 = slice(8 * i, 8 * i + 8)
                    linear = linear + positive[rows8]
                    product = factor[rows8] if product is None else product * factor[rows8]
                    count += 1
                    if count == GROUP:
                        logs = logs + jnp.log(product * 2.0 ** -GROUP)
                        product, count = None, 0
        blocks = []
        for q in range(4):
            total = None
            for h in range(2):
                pick = grads[h][8 * q:8 * q + 8]
                for j in range(1, 4):
                    pick = jnp.where(lane == j, grads[h][32 * j + 8 * q:32 * j + 8 * q + 8], pick)
                total = pick if total is None else total + pick
            blocks.append(total)
        message = None
        for k in range(4):
            turn = blocks[-k % 4]
            for j in range(1, 4):
                turn = jnp.where(lane == j, blocks[(j - k) % 4], turn)
            message = turn if k == 0 else message + pltpu.roll(turn, 128 - 32 * k, 1)
        outgoing[parity] = message

        def gradient_copy(k):
            return pltpu.make_async_remote_copy(src_ref=outgoing.at[parity, 0:MESSAGE], dst_ref=incoming.at[parity, k, 0:MESSAGE], send_sem=send_sem.at[parity], recv_sem=recv_sem.at[parity, k // 16], device_id=peer(OFFSETS[k]), device_id_type=pl.DeviceIdType.MESH)

        for k in FAR_FIRST:
            gradient_copy(k).start()

        loss = 2.0 * linear - logs
        loss = jnp.sum(loss[:, :128] + loss[:, 128:], axis=0, keepdims=True)
        loss_rows[pl.ds(loss_index + 7, 1), :] = lane_total(loss)

        def energy_copy(k):
            return pltpu.make_async_remote_copy(src_ref=energy_out, dst_ref=energy_in.at[k], send_sem=esend_sem.at[0], recv_sem=erecv_sem.at[k // 16], device_id=peer(OFFSETS[k]), device_id_type=pl.DeviceIdType.MESH)

        if last:
            own = loss_rows[8:24, :]
            for q in range(1, 4):
                own = jnp.where(lane16 == q, loss_rows[8 + 16 * q:24 + 16 * q, :], own)
            energy_out[...] = own
            for k in FAR_FIRST:
                energy_copy(k).start()

        def wait_planes(buffer, rows, sems):
            for plane in (0, 1, 3, 2):
                low = max(16 * plane, 1)
                ref = buffer.at[low:16 * plane + 16, 0:rows] if rows else buffer.at[low:16 * plane + 16]
                pltpu.make_async_copy(ref, ref, sems.at[plane]).wait()

        wait_planes(incoming.at[parity], MESSAGE, recv_sem.at[parity])
        total = ring_sum([message if k == 0 else incoming[parity, k] for k in range(64)])
        sent = incoming.at[parity, 1:64, 0:MESSAGE]
        pltpu.make_async_copy(sent, sent, send_sem.at[parity]).wait()
        gradient = jnp.where(real_row, -0.5 * total - positions / PRIOR_VAR, 0.0)
        if not last:
            return gradient
        wait_planes(energy_in, 0, erecv_sem)
        losses = ring_sum([energy_out[...] if k == 0 else energy_in[k] for k in range(64)])
        sent = energy_in.at[1:64]
        pltpu.make_async_copy(sent, sent, esend_sem.at[0]).wait()
        return gradient, losses

    def kinetic(positions, momentum, row):
        value = positions * positions / (2.0 * PRIOR_VAR) + 0.5 * (momentum * momentum)
        kin_rows[pl.ds(row + 7, 1), :] = lane_total(jnp.sum(value, axis=0, keepdims=True))

    def leap(number, parity, state, last=False):
        positions, momentum, gradient = state
        step_size = eps_ref[core, pl.ds(number, 1), :]
        momentum_half = momentum + 0.5 * step_size * gradient
        moved = positions + step_size * momentum_half
        result = evaluate(moved, parity, number, last)
        kinetic(positions, momentum, jnp.maximum(number - 1, 0))
        gradient = result[0] if last else result
        momentum = momentum_half + 0.5 * step_size * gradient
        if not last:
            return moved, momentum, gradient
        kinetic(moved, momentum, number)
        return moved, momentum, result[1]

    def two_leaps(i, state):
        return leap(2 * i + 1, 1, leap(2 * i, 0, state))

    state = (pos_ref[core], mom_ref[core], jnp.zeros((8, 128), jnp.float32))
    state = lax.fori_loop(0, STEPS // 2, two_leaps, state)
    positions, momentum, energy = leap(STEPS, 0, state, last=True)

    local = kin_rows[8:24, :]
    for q in range(1, 4):
        local = jnp.where(lane16 == q, kin_rows[8 + 16 * q:24 + 16 * q, :], local)
    final[core, 0:8, :] = positions
    final[core, 8:16, :] = momentum
    final[core, 16:32, :] = energy + local
    pair_copy(final, core, core, 2).start()
    pair_copy(final, core, core, 2).wait()
    out_ref[...] = final[...]


def to_lanes(array):
    split = array.reshape(4, 7, 2, HALF).transpose(2, 1, 0, 3).reshape(2, 7, 128)
    return jnp.pad(split, ((0, 0), (0, 1), (0, 0)))


def from_lanes(array):
    return array[:, :7].reshape(2, 7, 4, HALF).transpose(2, 1, 0, 3).reshape(FEATURES, CHAINS)


def solution(mesh):
    row_spec = P("data", None)
    chain_spec = P(None, "parts")

    def local_chains(feat_rows, labels, pos_init, mom_init, step_sizes):
        signed = feat_rows * (1 - 2 * labels).astype(jnp.bfloat16)[:, None]
        eps = jnp.pad(step_sizes, ((1, 7), (0, 0))).reshape(72, 2, 1, HALF)
        eps = jnp.broadcast_to(eps, (72, 2, 4, HALF)).transpose(1, 0, 2, 3).reshape(2, 72, 128)
        vmem = pl.BlockSpec(memory_space=pltpu.VMEM)
        final = pl.pallas_call(
            chain_kernel,
            out_shape=jax.ShapeDtypeStruct((2, 32, 128), jnp.float32),
            in_specs=[vmem] * 4,
            out_specs=vmem,
            scratch_shapes=[
                pltpu.VMEM((2, PROWS, 256), jnp.bfloat16),
                pltpu.VMEM((2, 256, PROWS), jnp.bfloat16),
                pltpu.VMEM((256, 256), jnp.bfloat16),
                pltpu.VMEM((16, 128), jnp.bfloat16),
                pltpu.VMEM((2, 8, 128), jnp.float32),
                pltpu.VMEM((2, 64, 8, 128), jnp.float32),
                pltpu.VMEM((80, 128), jnp.float32),
                pltpu.VMEM((80, 128), jnp.float32),
                pltpu.VMEM((16, 128), jnp.float32),
                pltpu.VMEM((64, 16, 128), jnp.float32),
                pltpu.VMEM((2, 32, 128), jnp.float32),
                pltpu.SemaphoreType.DMA((2,)),
                pltpu.SemaphoreType.DMA((2, 4)),
                pltpu.SemaphoreType.DMA((1,)),
                pltpu.SemaphoreType.DMA((4,)),
                pltpu.SemaphoreType.DMA((3,)),
                pltpu.SemaphoreType.DMA((3,)),
            ],
            compiler_params=pltpu.CompilerParams(has_side_effects=True),
            name="chains",
        )(signed, to_lanes(pos_init), to_lanes(mom_init), eps)
        energies = final[:, 16:32].reshape(2, 16, 4, HALF).transpose(2, 1, 0, 3).reshape(STEPS, CHAINS)
        return from_lanes(final[:, 0:8]), from_lanes(final[:, 8:16]), energies

    return jax.shard_map(local_chains, mesh=mesh, in_specs=(row_spec, P("data"), chain_spec, chain_spec, chain_spec), out_specs=(chain_spec, chain_spec, chain_spec), check_vma=False)
```
